32 devices in a mesh: tm: 8 (over z, x), env: 4 (over y, core).
Axes of the slice: x: 2, y: 2, z: 4, core: 2. Of those that a mesh axis runs over, the one named last changes fastest.
Arguments:
- init_state: float32 [70, 1024], P(None, 'env'), may hold values from -6 to 6
- torque: float32 [32, 35, 1024], P('tm', None, 'env'), may hold values from -192 to 192
- contact: int32 [32, 1024], P('tm', 'env'), may hold values 0 or 1
- mass_inverse: float32 [16, 35, 35], P('tm'), may hold values from -0.014 to 1.5, as said below
- stiffness: float32 [35], replicated, may hold values from 10 to 100
- damping: float32 [35], replicated, may hold values from 0.5 to 5
- gravity: float32 [35], replicated, may hold values from 1 to 10
- contact_stiffness: float32 [35], replicated, may hold values from 20 to 100
- contact_damping: float32 [35], replicated, may hold values from 0.5 to 3
Outputs:
- final_states: float32 [16, 70, 1024], P('tm', None, 'env')
- corrections: float32 [3, 1024], P(None, 'env')
The draws below stay inside these ranges and needn't reach their ends.
Inputs may be any that keep to these rules, and one draw needn't show every extreme that they name: `mass_inverse`: each matrix is symmetric, and each diagonal entry exceeds the sum of the magnitudes of the other entries of its row.
All inputs are finite; a program needn't handle non-finite values. No bound on the sum of `contact` on one device may be relied on, other than what follows from the above.
Results may differ from the reference program's by a relative error of at most 0.00025.
Values sent between devices are 32-bit elements; how exact they have to be, the bound alone decides.
A program may use at most 64 MiB of HBM per device.

```python
import math
import jax
import jax.numpy as jnp
from jax import lax

DOF = 35
STATE = 70
HS = 2
SUB = 32
ITERS = 3
SLICES = 16
STEPS = 32
ENV = 1024


def draw_mass_inverse(key, part):
    key_diag = jax.random.fold_in(key, 11)
    key_off = jax.random.fold_in(key, 12)
    diagonal = jax.random.uniform(key_diag, (SLICES, DOF), jnp.float32, 0.5, 1.5)
    raw = jnp.clip(0.008 * jax.random.normal(key_off, (SLICES, DOF, DOF), jnp.float32), -0.014, 0.014)
    upper = jnp.triu(raw, 1)
    return upper + jnp.swapaxes(upper, 1, 2) + diagonal[:, :, None] * jnp.eye(DOF, dtype=jnp.float32)


def touch_ends(values, own_key, low, largest):
    spot = [jax.random.randint(jax.random.fold_in(own_key, axis), (), 0, length) for axis, length in enumerate(values.shape)]
    widest = values.shape.index(max(values.shape))
    neighbour = spot[:widest] + [(spot[widest] + 1) % values.shape[widest]] + spot[widest + 1:]
    return values.at[tuple(spot)].set(low).at[tuple(neighbour)].set(largest)


def shard_levels(key, extent, cuts, low, largest):
    factor_of, own = 1.0, jax.random.fold_in(key, 6)
    for position, shards_of in cuts:
        draws = jnp.exp(jax.random.uniform(jax.random.fold_in(own, position), (shards_of,), jnp.float32, low / len(cuts), largest / len(cuts)))
        factor_of = factor_of * jnp.repeat(draws, extent[position] // shards_of).reshape([-1 if axis == position else 1 for axis in range(len(extent))])
    return factor_of


def gaussian(own_key, dims, deviation, most, shards=(), kind=jnp.bfloat16):
    array = jax.random.normal(own_key, dims, jnp.float32) * deviation
    if len(shards) > 0:
        array = shard_levels(own_key, dims, shards, -0.22, 0.18) * array
    return jnp.clip(array, min=-most, max=most).astype(kind)


def setup_inputs(seed: int = 0) -> dict:
    arg_keys = jax.random.split(jax.random.key(seed), 10)
    return {
        "init_state": gaussian(arg_keys[0], (STATE, ENV), 0.5, 6.0, ((1, 4),), jnp.float32),
        "torque": gaussian(arg_keys[1], (STEPS, DOF, ENV), 30.0, 192.0, ((0, 8), (2, 4)), jnp.float32),
        "contact": touch_ends((jax.random.randint(arg_keys[2], (STEPS, ENV), 0, 3) < 1).astype(jnp.int32), jax.random.fold_in(arg_keys[2], 1), 0, 1),
        "mass_inverse": draw_mass_inverse(jax.random.fold_in(arg_keys[9], 71), 0),
        "stiffness": jnp.clip(jnp.exp(jax.random.uniform(arg_keys[4], (DOF,), jnp.float32, math.log(10.0), math.log(100.0))), 10.0, 100.0),
        "damping": jnp.clip(jnp.exp(jax.random.uniform(arg_keys[5], (DOF,), jnp.float32, math.log(0.5), math.log(5.0))), 0.5, 5.0),
        "gravity": jnp.clip(jnp.exp(jax.random.uniform(arg_keys[6], (DOF,), jnp.float32, math.log(1.0), math.log(10.0))), 1.0, 10.0),
        "contact_stiffness": jnp.clip(jnp.exp(jax.random.uniform(arg_keys[7], (DOF,), jnp.float32, math.log(20.0), math.log(100.0))), 20.0, 100.0),
        "contact_damping": jnp.clip(jnp.exp(jax.random.uniform(arg_keys[8], (DOF,), jnp.float32, math.log(0.5), math.log(3.0))), 0.5, 3.0),
    }


step_length = 0.05

def exact_dot(left, right):
    return jnp.dot(left, right, precision=lax.Precision.HIGHEST, preferred_element_type=jnp.float32)

def coarse_one(state_now, torque_steps, mean_steps, inverse, params):
    stiffness, damping, gravity, contact_stiffness, contact_damping = params
    joint_pos = state_now[:DOF]
    joint_vel = state_now[DOF:]
    for step_pos in range(HS):
        spring = (stiffness + gravity + mean_steps[step_pos] * contact_stiffness)[:, None]
        friction = (damping + mean_steps[step_pos] * contact_damping)[:, None]
        force = torque_steps[step_pos] - spring * joint_pos - friction * joint_vel
        joint_vel = joint_vel + step_length * exact_dot(inverse, force)
        joint_pos = joint_pos + step_length * joint_vel
    return jnp.concatenate([joint_pos, joint_vel], axis=0)

def fine_one(state_now, torque_steps, contact_steps, inverse, params):
    stiffness, damping, gravity, contact_stiffness, contact_damping = params
    fine_dt = step_length / SUB
    joint_pair = (state_now[:DOF], state_now[DOF:])
    for step_pos in range(HS):
        torque_here = torque_steps[step_pos]
        contact_here = contact_steps[step_pos][None, :]

        def substep(counter, pair_now):
            joint_pos, joint_vel = pair_now
            force = torque_here - stiffness[:, None] * joint_pos - damping[:, None] * joint_vel - gravity[:, None] * jnp.sin(joint_pos) - contact_here * (contact_stiffness[:, None] * joint_pos + contact_damping[:, None] * joint_vel)
            joint_vel = joint_vel + fine_dt * exact_dot(inverse, force)
            joint_pos = joint_pos + fine_dt * joint_vel
            return (joint_pos, joint_vel)
        joint_pair = lax.fori_loop(0, SUB, substep, joint_pair)
    return jnp.concatenate([joint_pair[0], joint_pair[1]], axis=0)

def reference(init_state, torque, contact, mass_inverse, stiffness, damping, gravity, contact_stiffness, contact_damping):
    params = (stiffness, damping, gravity, contact_stiffness, contact_damping)
    torque_steps = torque.reshape(SLICES, HS, DOF, ENV)
    contact_steps = contact.astype(jnp.float32).reshape(SLICES, HS, ENV)
    mean_steps = lax.optimization_barrier(jnp.mean(contact_steps, axis=2))
    coarse_all = jax.vmap(coarse_one, in_axes=(0, 0, 0, 0, None))
    fine_all = jax.vmap(fine_one, in_axes=(0, 0, 0, 0, None))

    def chain(jumps):

        def advance(state_now, inputs):
            torque_here, mean_here, inverse, jump = inputs
            following = coarse_one(state_now, torque_here, mean_here, inverse, params) + jump
            return (following, following)
        unused, ends = lax.scan(advance, init_state, (torque_steps, mean_steps, mass_inverse, jumps))
        return ends
    ends = chain(jnp.zeros((SLICES, STATE, ENV), jnp.float32))
    records = []
    for iteration in range(ITERS):
        starts = jnp.concatenate([init_state[None], ends[:-1]], axis=0)
        jumps = fine_all(starts, torque_steps, contact_steps, mass_inverse, params) - coarse_all(starts, torque_steps, mean_steps, mass_inverse, params)
        new_ends = chain(jumps)
        records.append(lax.optimization_barrier(jnp.max(jnp.sqrt(lax.optimization_barrier(jnp.sum((new_ends - ends) ** 2, axis=1))), axis=0)))
        ends = new_ends
    return (ends, jnp.stack(records))
```

```python
import functools
import math

import jax
import jax.numpy as jnp
from jax import lax
from jax.experimental import pallas as pl
from jax.experimental.pallas import tpu as pltpu
from jax.sharding import PartitionSpec as P

DOF = 35
HS = 2
SUB = 32
ITERS = 3
LANES = 128
WIDE = 256

step_length = 0.05
fine_dt = step_length / SUB
TWO_PI = 2.0 * math.pi
MESH = pl.DeviceIdType.MESH
F32 = jnp.float32
BF16 = jnp.bfloat16

SIN = (
    6.283182818551188, -41.341421398631915, 81.59618387021051,
    -76.58010048603072, 41.205394649903326, -12.271261959178284,
)


def exchange_in(tm, env, tx, m2, row, rx, mall, rows, tsend, trecv, msend, mrecv, rsend, rrecv):
    me_t = lax.axis_index("tm")
    me_e = lax.axis_index("env")
    barrier = pltpu.get_barrier_semaphore()

    def peer(k):
        return {
            "tm": lax.rem(me_t + k // env, tm),
            "env": lax.rem(me_e + lax.rem(k, env), env),
        }

    @pl.loop(1, tm * env)
    def _(k):
        pl.semaphore_signal(barrier, inc=1, device_id=peer(k), device_id_type=MESH)

    pl.semaphore_wait(barrier, tm * env - 1)

    def row_copy(k):
        return pltpu.make_async_remote_copy(
            src_ref=row,
            dst_ref=rows.at[me_t, me_e],
            send_sem=rsend.at[k],
            recv_sem=rrecv.at[k],
            device_id=peer(k),
            device_id_type=MESH,
        )

    def pair(k):
        dst = lax.rem(me_t + k, tm)
        return (
            pltpu.make_async_remote_copy(
                src_ref=m2,
                dst_ref=mall.at[me_t],
                send_sem=msend.at[k],
                recv_sem=mrecv.at[k],
                device_id={"tm": dst, "env": me_e},
                device_id_type=MESH,
            ),
            pltpu.make_async_remote_copy(
                src_ref=tx.at[dst],
                dst_ref=rx.at[me_t],
                send_sem=tsend.at[k],
                recv_sem=trecv.at[k],
                device_id={"tm": dst, "env": me_e},
                device_id_type=MESH,
            ),
        )

    @pl.loop(1, tm * env)
    def _(k):
        row_copy(k).start()

    @pl.loop(1, tm)
    def _(k):
        first, second = pair(k)
        first.start()
        second.start()

    rows[me_t, me_e] = row[...]
    mall[me_t] = m2[...]
    rx[me_t] = tx[me_t]

    @pl.loop(1, tm * env)
    def _(k):
        row_copy(k).wait()

    @pl.loop(1, tm)
    def _(k):
        first, second = pair(k)
        first.wait()
        second.wait()


def exchange_out(tm, tx, rx, send, recv):
    me_t = lax.axis_index("tm")
    me_e = lax.axis_index("env")
    barrier = pltpu.get_barrier_semaphore()

    @pl.loop(1, tm)
    def _(k):
        dst = lax.rem(me_t + k, tm)
        pl.semaphore_signal(
            barrier, inc=1, device_id={"tm": dst, "env": me_e}, device_id_type=MESH
        )

    pl.semaphore_wait(barrier, tm - 1)

    def copy(k):
        dst = lax.rem(me_t + k, tm)
        return pltpu.make_async_remote_copy(
            src_ref=tx.at[dst],
            dst_ref=rx.at[me_t],
            send_sem=send.at[k],
            recv_sem=recv.at[k],
            device_id={"tm": dst, "env": me_e},
            device_id_type=MESH,
        )

    @pl.loop(1, tm)
    def _(k):
        copy(k).start()

    rx[me_t] = tx[me_t]

    @pl.loop(1, tm)
    def _(k):
        copy(k).wait()


def split(value):
    high = value.astype(BF16)
    return high, (value - high.astype(F32)).astype(BF16)


def dot(left, right):
    return jnp.dot(left, right, preferred_element_type=F32)


class Plan:
    def __init__(self, slices):
        per = WIDE // DOF
        self.groups = []
        self.where = []
        base = 0
        for first in range(0, slices, per):
            count = min(per, slices - first)
            width = -(-count * DOF // LANES) * LANES
            self.groups.append((base, width, first, count))
            for pos in range(count):
                self.where.append(base + pos * DOF)
            base += width
        self.lanes = base


def compute(
    slices, local, total_env,
    rx, mall, rows, start, prm,
    out,
    tq, spring, fric, grav, cspring, cfric, whi, wlo, wtmp, ybuf, ubuf, by, bu, ly, lu, cmap, ctmp, xs,
):
    plan = Plan(slices)
    epd = start.shape[0]
    ratio = float(SUB)
    stiff = prm[0:1, :]
    damp = prm[1:2, :]
    gravity = prm[2:3, :]
    cstiff = prm[3:4, :]
    cdamp = prm[4:5, :]
    to_u = TWO_PI / fine_dt

    for ref in (tq, spring, fric, grav, cspring, cfric, ybuf, ubuf, ly, lu):
        ref[...] = jnp.zeros(ref.shape, ref.dtype)
    ctmp[...] = jnp.zeros(ctmp.shape, F32)
    xs[...] = jnp.zeros(xs.shape, F32)

    sums = jnp.sum(rows[...], axis=1)[:, 0, :] * (1.0 / total_env)
    for n in range(slices):
        src, pos = divmod(n, local)
        at = plan.where[n]
        cut = pl.ds(at, DOF)
        grav[:, cut] = jnp.broadcast_to(gravity, (1, DOF))
        for j in range(HS):
            step = pos * HS + j
            lane = local * HS * DOF + step
            hit = rx[src, :, lane : lane + 1]
            mean = sums[src : src + 1, step : step + 1]
            tq[j, :, cut] = rx[src, :, step * DOF : (step + 1) * DOF]
            spring[j, :, cut] = TWO_PI * (stiff + hit * cstiff)
            fric[j, :, cut] = to_u * (damp + hit * cdamp)
            cspring[j, :, cut] = TWO_PI * (stiff + gravity + mean * cstiff)
            cfric[j, :, cut] = to_u * (damp + mean * cdamp)

    for g, (base, width, first, count) in enumerate(plan.groups):
        wtmp[...] = jnp.zeros(wtmp.shape, F32)
        for pos in range(count):
            src, here = divmod(first + pos, local)
            wtmp[pl.ds(pos * DOF, DOF), pl.ds(pos * DOF, DOF)] = (
                fine_dt * fine_dt / TWO_PI
            ) * mall[src, :, here * DOF : (here + 1) * DOF]
        high, low = split(wtmp[...])
        whi[g] = high
        wlo[g] = low

    def product(force, g, width):
        high, low = split(force)
        upper = whi[g, :width, :width]
        lower = wlo[g, :width, :width]
        return dot(high, upper) + dot(low, upper) + dot(high, lower)

    rank = lax.broadcasted_iota(jnp.int32, (ly.shape[0], DOF), 0)
    col = lax.broadcasted_iota(jnp.int32, (ly.shape[0], DOF), 1)
    for n in range(slices):
        cut = pl.ds(plan.where[n], DOF)
        ly[:, cut] = jnp.where(rank == col, 1.0, 0.0)
        lu[:, cut] = jnp.where(rank == col + DOF, 1.0, 0.0)
    for g, (base, width, first, count) in enumerate(plan.groups):
        cut = pl.ds(base, width)
        y, u = ly[:, cut], lu[:, cut]
        for j in range(HS):
            force = -cspring[j, :, cut] * y - cfric[j, :, cut] * u
            u = u + ratio * product(force, g, width)
            y = y + ratio * u
        ly[:, cut] = y
        lu[:, cut] = u
        u = ratio * product(tq[0, :, cut], g, width)
        y = ratio * u
        for j in range(1, HS):
            force = tq[j, :, cut] - cspring[j, :, cut] * y - cfric[j, :, cut] * u
            u = u + ratio * product(force, g, width)
            y = y + ratio * u
        by[:, cut] = y
        bu[:, cut] = u
    cmap[...] = jnp.zeros(cmap.shape, BF16)
    depth = ly.shape[0]
    for n in range(slices):
        cut = pl.ds(plan.where[n], DOF)
        ctmp[0:depth, 0:DOF] = ly[:, cut]
        ctmp[0:depth, DOF : 2 * DOF] = lu[:, cut]
        high, low = split(ctmp[...])
        cmap[n, 0:LANES, 0:LANES] = high
        cmap[n, LANES:, 0:LANES] = high
        cmap[n, 0:LANES, LANES:] = low

    def advance(state, n):
        high, low = split(state)
        both = dot(jnp.concatenate([high, low], axis=1), cmap[n])
        return both[:, :LANES] + both[:, LANES:]

    def packed(yref, uref, n):
        cut = pl.ds(plan.where[n], DOF)
        zero = jnp.zeros((epd, LANES - 2 * DOF), F32)
        return jnp.concatenate([yref[:, cut], uref[:, cut], zero], axis=1)

    state = start[...]
    xs[0] = state
    for n in range(slices):
        state = advance(state, n) + packed(by, bu, n)
        xs[n + 1] = state

    lane_of = lax.broadcasted_iota(jnp.int32, (1, LANES), 1)
    scale = jnp.where(lane_of < DOF, TWO_PI, to_u)

    def iteration(k, corrections):
        for n in range(slices):
            cut = pl.ds(plan.where[n], DOF)
            ybuf[:, cut] = xs[n, :, 0:DOF]
            ubuf[:, cut] = xs[n, :, DOF : 2 * DOF]
        for j in range(HS):

            def substep(counter, carry):
                result = []
                for g, (base, width, first, count) in enumerate(plan.groups):
                    y, u = carry[g]
                    cut = pl.ds(base, width)
                    t = y - jnp.round(y)
                    s = t * t
                    poly = jnp.full_like(s, SIN[-1])
                    for c in SIN[-2::-1]:
                        poly = poly * s + c
                    force = (
                        tq[j, :, cut]
                        - spring[j, :, cut] * y
                        - fric[j, :, cut] * u
                        - (grav[:, cut] * t) * poly
                    )
                    u = u + product(force, g, width)
                    y = y + u
                    result.append((y, u))
                return tuple(result)

            first_state = tuple(
                (ybuf[:, pl.ds(base, width)], ubuf[:, pl.ds(base, width)])
                for base, width, first, count in plan.groups
            )
            last = lax.fori_loop(0, SUB, substep, first_state)
            for g, (base, width, first, count) in enumerate(plan.groups):
                ybuf[:, pl.ds(base, width)] = last[g][0]
                ubuf[:, pl.ds(base, width)] = last[g][1]
        worst = jnp.zeros((epd, 1), F32)
        change = None
        for n in range(slices):
            jump = packed(ybuf, ubuf, n) - xs[n + 1]
            change = jump if change is None else advance(change, n) + jump
            real = change * scale
            worst = jnp.maximum(worst, jnp.sum(real * real, axis=1, keepdims=True))
            xs[n + 1] = xs[n + 1] + change
        return jnp.where(lane_of == k, jnp.sqrt(worst), corrections)

    corrections = lax.fori_loop(0, ITERS, iteration, jnp.zeros((epd, LANES), F32))
    rows_of = 2 * DOF
    for n in range(slices):
        dst, pos = divmod(n, local)
        out[dst, :, pos * rows_of : (pos + 1) * rows_of] = (xs[n + 1] * scale)[:, :rows_of]
    for dst in range(slices // local):
        out[dst, :, local * rows_of : local * rows_of + ITERS] = corrections[:, :ITERS]


def body(tm, env, init_state, torque, contact, mass_inverse, stiffness, damping, gravity,
         contact_stiffness, contact_damping):
    local = mass_inverse.shape[0]
    steps = torque.shape[0]
    env_local = init_state.shape[1]
    epd = env_local // tm
    slices = local * tm
    plan = Plan(slices)
    vmem = pl.BlockSpec(memory_space=pltpu.VMEM)
    dma = pltpu.SemaphoreType.DMA

    flat = jnp.concatenate(
        [torque.reshape(steps * DOF, env_local), contact.astype(F32)], axis=0
    ).T
    wide = flat.shape[1]
    tx = flat.reshape(tm, epd, wide)
    m2 = mass_inverse.transpose(1, 0, 2).reshape(DOF, local * DOF)
    row = jnp.pad(jnp.sum(contact.astype(F32), axis=1)[None], ((0, 0), (0, LANES - steps)))
    rx, mall, rows = pl.pallas_call(
        functools.partial(exchange_in, tm, env),
        out_shape=(
            jax.ShapeDtypeStruct(tx.shape, F32),
            jax.ShapeDtypeStruct((tm,) + m2.shape, F32),
            jax.ShapeDtypeStruct((tm, env, 1, LANES), F32),
        ),
        in_specs=[vmem] * 3,
        out_specs=(vmem,) * 3,
        scratch_shapes=[dma((tm,))] * 4 + [dma((tm * env,))] * 2,
        compiler_params=pltpu.CompilerParams(collective_id=0, has_side_effects=True),
        name="exchange_in",
    )(tx, m2, row)

    me_t = lax.axis_index("tm")
    mine = lax.dynamic_slice_in_dim(init_state, me_t * epd, epd, axis=1)
    unit = jnp.concatenate([
        jnp.full((DOF, 1), 1.0 / TWO_PI, F32), jnp.full((DOF, 1), fine_dt / TWO_PI, F32)
    ])
    start = jnp.pad((mine * unit).T, ((0, 0), (0, LANES - 2 * DOF)))
    prm = jnp.stack([stiffness, damping, gravity, contact_stiffness, contact_damping])
    depth = -(-2 * DOF // 8) * 8
    lanes = plan.lanes
    groups = len(plan.groups)
    width_out = local * 2 * DOF + ITERS
    big = pltpu.VMEM((epd, lanes), F32)
    both = pltpu.VMEM((HS, epd, lanes), F32)
    thin = pltpu.VMEM((HS, 1, lanes), F32)
    out = pl.pallas_call(
        functools.partial(compute, slices, local, env_local * env),
        out_shape=jax.ShapeDtypeStruct((tm, epd, width_out), F32),
        in_specs=[vmem] * 5,
        out_specs=vmem,
        scratch_shapes=[
            both, both, both, pltpu.VMEM((1, lanes), F32), thin, thin,
            pltpu.VMEM((groups, WIDE, WIDE), BF16), pltpu.VMEM((groups, WIDE, WIDE), BF16),
            pltpu.VMEM((WIDE, WIDE), F32),
            big, big, big, big,
            pltpu.VMEM((depth, lanes), F32), pltpu.VMEM((depth, lanes), F32),
            pltpu.VMEM((slices, 2 * LANES, 2 * LANES), BF16),
            pltpu.VMEM((LANES, LANES), F32),
            pltpu.VMEM((slices + 1, epd, LANES), F32),
        ],
        name="parareal",
    )(rx, mall, rows, start, prm)

    back = pl.pallas_call(
        functools.partial(exchange_out, tm),
        out_shape=jax.ShapeDtypeStruct(out.shape, F32),
        in_specs=[vmem],
        out_specs=vmem,
        scratch_shapes=[dma((tm,))] * 2,
        compiler_params=pltpu.CompilerParams(collective_id=1, has_side_effects=True),
        name="exchange_out",
    )(out)
    turned = back.reshape(env_local, width_out).T
    states = turned[: local * 2 * DOF].reshape(local, 2 * DOF, env_local)
    return states, turned[local * 2 * DOF :]


def solution(mesh):
    placed = (
        P(None, "env"),
        P("tm", None, "env"),
        P("tm", "env"),
        P("tm", None, None),
        P(),
        P(),
        P(),
        P(),
        P(),
    )
    return jax.shard_map(
        functools.partial(body, mesh.shape["tm"], mesh.shape["env"]),
        mesh=mesh,
        in_specs=placed,
        out_specs=(P("tm", None, "env"), P(None, "env")),
        check_vma=False,
    )
```

```python
import functools
import math

import jax
import jax.numpy as jnp
from jax import lax
from jax.experimental import pallas as pl
from jax.experimental.pallas import tpu as pltpu
from jax.sharding import PartitionSpec as P

DOF = 35
HS = 2
SUB = 32
ITERS = 3
LANES = 128
WIDE = 256

step_length = 0.05
fine_dt = step_length / SUB
TWO_PI = 2.0 * math.pi
MESH = pl.DeviceIdType.MESH
F32 = jnp.float32
BF16 = jnp.bfloat16

SIN = (
    6.283182818551188, -41.341421398631915, 81.59618387021051,
    -76.58010048603072, 41.205394649903326, -12.271261959178284,
)


def exchange_in(tm, env, tx, m2, row, rx, mall, rows, tsend, trecv, msend, mrecv, rsend, rrecv):
    me_t = lax.axis_index("tm")
    me_e = lax.axis_index("env")
    barrier = pltpu.get_barrier_semaphore()

    def peer(k):
        return {
            "tm": lax.rem(me_t + k // env, tm),
            "env": lax.rem(me_e + lax.rem(k, env), env),
        }

    @pl.loop(1, tm * env)
    def _(k):
        pl.semaphore_signal(barrier, inc=1, device_id=peer(k), device_id_type=MESH)

    pl.semaphore_wait(barrier, tm * env - 1)

    def row_copy(k):
        return pltpu.make_async_remote_copy(
            src_ref=row,
            dst_ref=rows.at[me_t, me_e],
            send_sem=rsend.at[k],
            recv_sem=rrecv.at[k],
            device_id=peer(k),
            device_id_type=MESH,
        )

    def pair(k):
        dst = lax.rem(me_t + k, tm)
        return (
            pltpu.make_async_remote_copy(
                src_ref=m2,
                dst_ref=mall.at[me_t],
                send_sem=msend.at[k],
                recv_sem=mrecv.at[k],
                device_id={"tm": dst, "env": me_e},
                device_id_type=MESH,
            ),
            pltpu.make_async_remote_copy(
                src_ref=tx.at[dst],
                dst_ref=rx.at[me_t],
                send_sem=tsend.at[k],
                recv_sem=trecv.at[k],
                device_id={"tm": dst, "env": me_e},
                device_id_type=MESH,
            ),
        )

    @pl.loop(1, tm * env)
    def _(k):
        row_copy(k).start()

    @pl.loop(1, tm)
    def _(k):
        first, second = pair(k)
        first.start()
        second.start()

    rows[me_t, me_e] = row[...]
    mall[me_t] = m2[...]
    rx[me_t] = tx[me_t]

    @pl.loop(1, tm * env)
    def _(k):
        row_copy(k).wait()

    @pl.loop(1, tm)
    def _(k):
        first, second = pair(k)
        first.wait()
        second.wait()


def exchange_out(tm, tx, rx, send, recv):
    me_t = lax.axis_index("tm")
    me_e = lax.axis_index("env")
    barrier = pltpu.get_barrier_semaphore()

    @pl.loop(1, tm)
    def _(k):
        dst = lax.rem(me_t + k, tm)
        pl.semaphore_signal(
            barrier, inc=1, device_id={"tm": dst, "env": me_e}, device_id_type=MESH
        )

    pl.semaphore_wait(barrier, tm - 1)

    def copy(k):
        dst = lax.rem(me_t + k, tm)
        return pltpu.make_async_remote_copy(
            src_ref=tx.at[dst],
            dst_ref=rx.at[me_t],
            send_sem=send.at[k],
            recv_sem=recv.at[k],
            device_id={"tm": dst, "env": me_e},
            device_id_type=MESH,
        )

    @pl.loop(1, tm)
    def _(k):
        copy(k).start()

    rx[me_t] = tx[me_t]

    @pl.loop(1, tm)
    def _(k):
        copy(k).wait()


def split(value):
    high = value.astype(BF16)
    return high, (value - high.astype(F32)).astype(BF16)


def dot(left, right):
    return jnp.dot(left, right, preferred_element_type=F32)


class Plan:
    def __init__(self, slices):
        per = LANES // DOF
        self.groups = []
        self.where = []
        base = 0
        for first in range(0, slices, per):
            count = min(per, slices - first)
            width = -(-count * DOF // LANES) * LANES
            self.groups.append((base, width, first, count))
            for pos in range(count):
                self.where.append(base + pos * DOF)
            base += width
        self.lanes = base


def compute(
    slices, local, total_env,
    rx, mall, rows, stiff, damp, gravity, cstiff, cdamp,
    out,
    tq, spring, fric, grav, cspring, cfric, wgt, wtmp, ybuf, ubuf, by, bu, ly, lu, cmap, ctmp, xs,
):
    plan = Plan(slices)
    epd = rx.shape[1]
    ratio = float(SUB)
    unroll = max(1, min(SUB, 48 // len(plan.groups)))
    stiff, damp, gravity, cstiff, cdamp = (r[...] for r in (stiff, damp, gravity, cstiff, cdamp))
    to_u = TWO_PI / fine_dt

    for ref in (tq, spring, fric, grav, cspring, cfric, ybuf, ubuf, ly, lu):
        ref[...] = jnp.zeros(ref.shape, ref.dtype)
    ctmp[...] = jnp.zeros(ctmp.shape, F32)
    xs[...] = jnp.zeros(xs.shape, F32)

    sums = jnp.sum(rows[...], axis=1)[:, 0, :] * (1.0 / total_env)
    for n in range(slices):
        src, pos = divmod(n, local)
        at = plan.where[n]
        cut = pl.ds(at, DOF)
        grav[:, cut] = jnp.broadcast_to(gravity, (1, DOF))
        for j in range(HS):
            step = pos * HS + j
            lane = local * HS * DOF + step
            hit = rx[src, :, lane : lane + 1]
            mean = sums[src : src + 1, step : step + 1]
            tq[j, :, cut] = rx[src, :, step * DOF : (step + 1) * DOF]
            spring[j, :, cut] = TWO_PI * (stiff + hit * cstiff)
            fric[j, :, cut] = to_u * (damp + hit * cdamp)
            cspring[j, :, cut] = TWO_PI * (stiff + gravity + mean * cstiff)
            cfric[j, :, cut] = to_u * (damp + mean * cdamp)

    for g, (base, width, first, count) in enumerate(plan.groups):
        wtmp[...] = jnp.zeros(wtmp.shape, F32)
        for pos in range(count):
            src, here = divmod(first + pos, local)
            wtmp[pl.ds(pos * DOF, DOF), pl.ds(pos * DOF, DOF)] = (
                fine_dt * fine_dt / TWO_PI
            ) * mall[src, :, here * DOF : (here + 1) * DOF]
        high, low = split(wtmp[...])
        wgt[g, 0:LANES, 0:LANES] = high
        wgt[g, LANES:, 0:LANES] = high
        wgt[g, 0:LANES, LANES:] = low
        wgt[g, LANES:, LANES:] = jnp.zeros_like(low)

    def product(force, g, width):
        high, low = split(force)
        both = dot(jnp.concatenate([high, low], axis=1), wgt[g])
        return both[:, :LANES] + both[:, LANES:]

    rank = lax.broadcasted_iota(jnp.int32, (ly.shape[0], DOF), 0)
    col = lax.broadcasted_iota(jnp.int32, (ly.shape[0], DOF), 1)
    for n in range(slices):
        cut = pl.ds(plan.where[n], DOF)
        ly[:, cut] = jnp.where(rank == col, 1.0, 0.0)
        lu[:, cut] = jnp.where(rank == col + DOF, 1.0, 0.0)
    for g, (base, width, first, count) in enumerate(plan.groups):
        cut = pl.ds(base, width)
        y, u = ly[:, cut], lu[:, cut]
        for j in range(HS):
            force = -cspring[j, :, cut] * y - cfric[j, :, cut] * u
            u = u + ratio * product(force, g, width)
            y = y + ratio * u
        ly[:, cut] = y
        lu[:, cut] = u
        u = ratio * product(tq[0, :, cut], g, width)
        y = ratio * u
        for j in range(1, HS):
            force = tq[j, :, cut] - cspring[j, :, cut] * y - cfric[j, :, cut] * u
            u = u + ratio * product(force, g, width)
            y = y + ratio * u
        by[:, cut] = y
        bu[:, cut] = u
    cmap[...] = jnp.zeros(cmap.shape, BF16)
    depth = ly.shape[0]
    for n in range(slices):
        cut = pl.ds(plan.where[n], DOF)
        ctmp[0:depth, 0:DOF] = ly[:, cut]
        ctmp[0:depth, DOF : 2 * DOF] = lu[:, cut]
        high, low = split(ctmp[...])
        cmap[n, 0:LANES, 0:LANES] = high
        cmap[n, LANES:, 0:LANES] = high
        cmap[n, 0:LANES, LANES:] = low

    def advance(state, n):
        high, low = split(state)
        both = dot(jnp.concatenate([high, low], axis=1), cmap[n])
        return both[:, :LANES] + both[:, LANES:]

    def packed(yref, uref, n):
        cut = pl.ds(plan.where[n], DOF)
        zero = jnp.zeros((epd, LANES - 2 * DOF), F32)
        return jnp.concatenate([yref[:, cut], uref[:, cut], zero], axis=1)

    lane_of = lax.broadcasted_iota(jnp.int32, (1, LANES), 1)
    scale = jnp.where(lane_of < DOF, TWO_PI, to_u)
    shrink = jnp.where(lane_of < DOF, 1.0 / TWO_PI, 1.0 / to_u)
    first_lane = local * HS * (DOF + 1)
    own = rx[lax.axis_index("tm")][:, first_lane : first_lane + 2 * DOF]
    state = jnp.concatenate([own, jnp.zeros((epd, LANES - 2 * DOF), F32)], axis=1) * shrink
    xs[0] = state
    for n in range(slices):
        state = advance(state, n) + packed(by, bu, n)
        xs[n + 1] = state

    def iteration(k, corrections):
        for n in range(slices):
            cut = pl.ds(plan.where[n], DOF)
            ybuf[:, cut] = xs[n, :, 0:DOF]
            ubuf[:, cut] = xs[n, :, DOF : 2 * DOF]
        for j in range(HS):

            def substep(counter, carry):
                result = []
                for g, (base, width, first, count) in enumerate(plan.groups):
                    y, u = carry[g]
                    cut = pl.ds(base, width)
                    t = y - jnp.round(y)
                    s = t * t
                    poly = jnp.full_like(s, SIN[-1])
                    for c in SIN[-2::-1]:
                        poly = poly * s + c
                    force = (
                        tq[j, :, cut]
                        - spring[j, :, cut] * y
                        - fric[j, :, cut] * u
                        - (grav[:, cut] * t) * poly
                    )
                    u = u + product(force, g, width)
                    y = y + u
                    result.append((y, u))
                return tuple(result)

            first_state = tuple(
                (ybuf[:, pl.ds(base, width)], ubuf[:, pl.ds(base, width)])
                for base, width, first, count in plan.groups
            )
            last = lax.fori_loop(0, SUB, substep, first_state, unroll=unroll)
            for g, (base, width, first, count) in enumerate(plan.groups):
                ybuf[:, pl.ds(base, width)] = last[g][0]
                ubuf[:, pl.ds(base, width)] = last[g][1]
        worst = jnp.zeros((epd, 1), F32)
        change = None
        for n in range(slices):
            jump = packed(ybuf, ubuf, n) - xs[n + 1]
            change = jump if change is None else advance(change, n) + jump
            real = change * scale
            worst = jnp.maximum(worst, jnp.sum(real * real, axis=1, keepdims=True))
            xs[n + 1] = xs[n + 1] + change
        return jnp.where(lane_of == k, jnp.sqrt(worst), corrections)

    corrections = lax.fori_loop(0, ITERS, iteration, jnp.zeros((epd, LANES), F32))
    rows_of = 2 * DOF
    for n in range(slices):
        dst, pos = divmod(n, local)
        out[dst, :, pos * rows_of : (pos + 1) * rows_of] = (xs[n + 1] * scale)[:, :rows_of]
    for dst in range(slices // local):
        out[dst, :, local * rows_of : local * rows_of + ITERS] = corrections[:, :ITERS]


def body(tm, env, init_state, torque, contact, mass_inverse, stiffness, damping, gravity,
         contact_stiffness, contact_damping):
    local = mass_inverse.shape[0]
    steps = torque.shape[0]
    env_local = init_state.shape[1]
    epd = env_local // tm
    slices = local * tm
    plan = Plan(slices)
    vmem = pl.BlockSpec(memory_space=pltpu.VMEM)
    dma = pltpu.SemaphoreType.DMA

    flat = jnp.concatenate(
        [torque.reshape(steps * DOF, env_local), contact.astype(F32), init_state], axis=0
    ).T
    wide = flat.shape[1]
    tx = flat.reshape(tm, epd, wide)
    m2 = mass_inverse.transpose(1, 0, 2).reshape(DOF, local * DOF)
    row = jnp.pad(jnp.sum(contact.astype(F32), axis=1)[None], ((0, 0), (0, LANES - steps)))
    rx, mall, rows = pl.pallas_call(
        functools.partial(exchange_in, tm, env),
        out_shape=(
            jax.ShapeDtypeStruct(tx.shape, F32),
            jax.ShapeDtypeStruct((tm,) + m2.shape, F32),
            jax.ShapeDtypeStruct((tm, env, 1, LANES), F32),
        ),
        in_specs=[vmem] * 3,
        out_specs=(vmem,) * 3,
        scratch_shapes=[dma((tm,))] * 4 + [dma((tm * env,))] * 2,
        compiler_params=pltpu.CompilerParams(collective_id=0, has_side_effects=True),
        name="exchange_in",
    )(tx, m2, row)

    prm = [p.reshape(1, DOF) for p in (stiffness, damping, gravity, contact_stiffness, contact_damping)]
    depth = -(-2 * DOF // 8) * 8
    lanes = plan.lanes
    groups = len(plan.groups)
    width_out = local * 2 * DOF + ITERS
    big = pltpu.VMEM((epd, lanes), F32)
    both = pltpu.VMEM((HS, epd, lanes), F32)
    thin = pltpu.VMEM((HS, 1, lanes), F32)
    out = pl.pallas_call(
        functools.partial(compute, slices, local, env_local * env),
        out_shape=jax.ShapeDtypeStruct((tm, epd, width_out), F32),
        in_specs=[vmem] * 8,
        out_specs=vmem,
        scratch_shapes=[
            both, both, both, pltpu.VMEM((1, lanes), F32), thin, thin,
            pltpu.VMEM((groups, WIDE, WIDE), BF16),
            pltpu.VMEM((LANES, LANES), F32),
            big, big, big, big,
            pltpu.VMEM((depth, lanes), F32), pltpu.VMEM((depth, lanes), F32),
            pltpu.VMEM((slices, 2 * LANES, 2 * LANES), BF16),
            pltpu.VMEM((LANES, LANES), F32),
            pltpu.VMEM((slices + 1, epd, LANES), F32),
        ],
        name="parareal",
    )(rx, mall, rows, *prm)

    back = pl.pallas_call(
        functools.partial(exchange_out, tm),
        out_shape=jax.ShapeDtypeStruct(out.shape, F32),
        in_specs=[vmem],
        out_specs=vmem,
        scratch_shapes=[dma((tm,))] * 2,
        compiler_params=pltpu.CompilerParams(collective_id=1, has_side_effects=True),
        name="exchange_out",
    )(out)
    turned = back.reshape(env_local, width_out).T
    states = turned[: local * 2 * DOF].reshape(local, 2 * DOF, env_local)
    return states, turned[local * 2 * DOF :]


def solution(mesh):
    placed = (
        P(None, "env"),
        P("tm", None, "env"),
        P("tm", "env"),
        P("tm", None, None),
        P(),
        P(),
        P(),
        P(),
        P(),
    )
    return jax.shard_map(
        functools.partial(body, mesh.shape["tm"], mesh.shape["env"]),
        mesh=mesh,
        in_specs=placed,
        out_specs=(P("tm", None, "env"), P(None, "env")),
        check_vma=False,
    )
```

```python
import functools
import math

import jax
import jax.numpy as jnp
from jax import lax
from jax.experimental import pallas as pl
from jax.experimental.pallas import tpu as pltpu
from jax.sharding import PartitionSpec as P

DOF = 35
HS = 2
SUB = 32
ITERS = 3
LANES = 128
WIDE = 256

step_length = 0.05
fine_dt = step_length / SUB
TWO_PI = 2.0 * math.pi
MESH = pl.DeviceIdType.MESH
F32 = jnp.float32
BF16 = jnp.bfloat16

SIN = (
    6.283182818551188, -41.341421398631915, 81.59618387021051,
    -76.58010048603072, 41.205394649903326, -12.271261959178284,
)


def exchange_in(tm, env, tx, m2, row, rx, mall, rows, tsend, trecv, msend, mrecv, rsend, rrecv):
    me_t = lax.axis_index("tm")
    me_e = lax.axis_index("env")
    barrier = pltpu.get_barrier_semaphore()

    def peer(k):
        return {
            "tm": lax.rem(me_t + k // env, tm),
            "env": lax.rem(me_e + lax.rem(k, env), env),
        }

    @pl.loop(1, tm * env)
    def _(k):
        pl.semaphore_signal(barrier, inc=1, device_id=peer(k), device_id_type=MESH)

    pl.semaphore_wait(barrier, tm * env - 1)

    def row_copy(k):
        return pltpu.make_async_remote_copy(
            src_ref=row,
            dst_ref=rows.at[me_t, me_e],
            send_sem=rsend.at[k],
            recv_sem=rrecv.at[k],
            device_id=peer(k),
            device_id_type=MESH,
        )

    def pair(k):
        dst = lax.rem(me_t + k, tm)
        return (
            pltpu.make_async_remote_copy(
                src_ref=m2,
                dst_ref=mall.at[me_t],
                send_sem=msend.at[k],
                recv_sem=mrecv.at[k],
                device_id={"tm": dst, "env": me_e},
                device_id_type=MESH,
            ),
            pltpu.make_async_remote_copy(
                src_ref=tx.at[dst],
                dst_ref=rx.at[me_t],
                send_sem=tsend.at[k],
                recv_sem=trecv.at[k],
                device_id={"tm": dst, "env": me_e},
                device_id_type=MESH,
            ),
        )

    @pl.loop(1, tm * env)
    def _(k):
        row_copy(k).start()

    @pl.loop(1, tm)
    def _(k):
        first, second = pair(k)
        first.start()
        second.start()

    rows[me_t, me_e] = row[...]
    mall[me_t] = m2[...]
    rx[me_t] = tx[me_t]

    @pl.loop(1, tm * env)
    def _(k):
        row_copy(k).wait()

    @pl.loop(1, tm)
    def _(k):
        first, second = pair(k)
        first.wait()
        second.wait()


def exchange_out(tm, tx, rx, send, recv):
    me_t = lax.axis_index("tm")
    me_e = lax.axis_index("env")
    barrier = pltpu.get_barrier_semaphore()

    @pl.loop(1, tm)
    def _(k):
        dst = lax.rem(me_t + k, tm)
        pl.semaphore_signal(
            barrier, inc=1, device_id={"tm": dst, "env": me_e}, device_id_type=MESH
        )

    pl.semaphore_wait(barrier, tm - 1)

    def copy(k):
        dst = lax.rem(me_t + k, tm)
        return pltpu.make_async_remote_copy(
            src_ref=tx.at[dst],
            dst_ref=rx.at[me_t],
            send_sem=send.at[k],
            recv_sem=recv.at[k],
            device_id={"tm": dst, "env": me_e},
            device_id_type=MESH,
        )

    @pl.loop(1, tm)
    def _(k):
        copy(k).start()

    rx[me_t] = tx[me_t]

    @pl.loop(1, tm)
    def _(k):
        copy(k).wait()


def split(value):
    high = value.astype(BF16)
    return high, (value - high.astype(F32)).astype(BF16)


def dot(left, right):
    return jnp.dot(left, right, preferred_element_type=F32)


class Plan:
    def __init__(self, slices):
        per = LANES // DOF
        self.groups = []
        self.where = []
        base = 0
        for first in range(0, slices, per):
            count = min(per, slices - first)
            width = -(-count * DOF // LANES) * LANES
            self.groups.append((base, width, first, count))
            for pos in range(count):
                self.where.append(base + pos * DOF)
            base += width
        self.lanes = base


def compute(
    slices, local, total_env,
    rx, mall, rows, stiff, damp, gravity, cstiff, cdamp,
    out,
    tq, spring, fric, grav, cspring, cfric, wgt, wtmp, ybuf, ubuf, by, bu, ly, lu, cmap, pmap, ctmp, xs,
):
    plan = Plan(slices)
    epd = rx.shape[1]
    ratio = float(SUB)
    block = 4 if slices % 4 == 0 else 1
    unroll = max(1, min(SUB, 96 // len(plan.groups)))
    stiff, damp, gravity, cstiff, cdamp = (r[...] for r in (stiff, damp, gravity, cstiff, cdamp))
    to_u = TWO_PI / fine_dt

    for ref in (tq, spring, fric, grav, cspring, cfric, ybuf, ubuf, ly, lu):
        ref[...] = jnp.zeros(ref.shape, ref.dtype)
    ctmp[...] = jnp.zeros(ctmp.shape, F32)
    xs[...] = jnp.zeros(xs.shape, F32)

    sums = jnp.sum(rows[...], axis=1)[:, 0, :] * (1.0 / total_env)
    for n in range(slices):
        src, pos = divmod(n, local)
        at = plan.where[n]
        cut = pl.ds(at, DOF)
        grav[:, cut] = jnp.broadcast_to(gravity, (1, DOF))
        for j in range(HS):
            step = pos * HS + j
            lane = local * HS * DOF + step
            hit = rx[src, :, lane : lane + 1]
            mean = sums[src : src + 1, step : step + 1]
            tq[j, :, cut] = rx[src, :, step * DOF : (step + 1) * DOF]
            spring[j, :, cut] = TWO_PI * (stiff + hit * cstiff)
            fric[j, :, cut] = to_u * (damp + hit * cdamp)
            cspring[j, :, cut] = TWO_PI * (stiff + gravity + mean * cstiff)
            cfric[j, :, cut] = to_u * (damp + mean * cdamp)

    for g, (base, width, first, count) in enumerate(plan.groups):
        wtmp[...] = jnp.zeros(wtmp.shape, F32)
        for pos in range(count):
            src, here = divmod(first + pos, local)
            wtmp[pl.ds(pos * DOF, DOF), pl.ds(pos * DOF, DOF)] = (
                fine_dt * fine_dt / TWO_PI
            ) * mall[src, :, here * DOF : (here + 1) * DOF]
        high, low = split(wtmp[...])
        wgt[g, 0:LANES, 0:LANES] = high
        wgt[g, LANES:, 0:LANES] = high
        wgt[g, 0:LANES, LANES:] = low
        wgt[g, LANES:, LANES:] = jnp.zeros_like(low)

    def product(force, g, width):
        high, low = split(force)
        both = dot(jnp.concatenate([high, low], axis=1), wgt[g])
        return both[:, :LANES] + both[:, LANES:]

    rank = lax.broadcasted_iota(jnp.int32, (ly.shape[0], DOF), 0)
    col = lax.broadcasted_iota(jnp.int32, (ly.shape[0], DOF), 1)
    for n in range(slices):
        cut = pl.ds(plan.where[n], DOF)
        ly[:, cut] = jnp.where(rank == col, 1.0, 0.0)
        lu[:, cut] = jnp.where(rank == col + DOF, 1.0, 0.0)
    for g, (base, width, first, count) in enumerate(plan.groups):
        cut = pl.ds(base, width)
        y, u = ly[:, cut], lu[:, cut]
        for j in range(HS):
            force = -cspring[j, :, cut] * y - cfric[j, :, cut] * u
            u = u + ratio * product(force, g, width)
            y = y + ratio * u
        ly[:, cut] = y
        lu[:, cut] = u
        u = ratio * product(tq[0, :, cut], g, width)
        y = ratio * u
        for j in range(1, HS):
            force = tq[j, :, cut] - cspring[j, :, cut] * y - cfric[j, :, cut] * u
            u = u + ratio * product(force, g, width)
            y = y + ratio * u
        by[:, cut] = y
        bu[:, cut] = u
    cmap[...] = jnp.zeros(cmap.shape, BF16)
    depth = ly.shape[0]
    for n in range(slices):
        cut = pl.ds(plan.where[n], DOF)
        ctmp[0:depth, 0:DOF] = ly[:, cut]
        ctmp[0:depth, DOF : 2 * DOF] = lu[:, cut]
        high, low = split(ctmp[...])
        cmap[n, 0:LANES, 0:LANES] = high
        cmap[n, LANES:, 0:LANES] = high
        cmap[n, 0:LANES, LANES:] = low

    def through(state, weight):
        high, low = split(state)
        both = dot(jnp.concatenate([high, low], axis=1), weight)
        return both[:, :LANES] + both[:, LANES:]

    firsts = range(0, slices, block)
    running = {m: jnp.concatenate(
        [ly[:, pl.ds(plan.where[m], DOF)], lu[:, pl.ds(plan.where[m], DOF)],
         jnp.zeros((depth, LANES - 2 * DOF), F32)], axis=1) for m in firsts}
    for i in range(1, block):
        for m in firsts:
            running[m] = through(running[m], cmap[m + i])
            ctmp[0:depth, :] = running[m]
            high, low = split(ctmp[...])
            pmap[m + i, 0:LANES, 0:LANES] = high
            pmap[m + i, LANES:, 0:LANES] = high
            pmap[m + i, 0:LANES, LANES:] = low
            pmap[m + i, LANES:, LANES:] = jnp.zeros_like(low)

    def sweep(offsets, entry):
        ends = list(offsets)
        for i in range(1, block):
            for m in firsts:
                ends[m + i] = through(ends[m + i - 1], cmap[m + i]) + ends[m + i]
        enter = {}
        for m in firsts:
            enter[m] = entry
            last = m + block - 1
            whole = pmap if block > 1 else cmap
            if entry is not None:
                ends[last] = ends[last] + through(entry, whole[last])
            entry = ends[last]
        for i in range(block - 1):
            for m in firsts:
                if enter[m] is not None:
                    part = cmap if i == 0 else pmap
                    ends[m + i] = ends[m + i] + through(enter[m], part[m + i])
        return ends

    def packed(yref, uref, n):
        cut = pl.ds(plan.where[n], DOF)
        zero = jnp.zeros((epd, LANES - 2 * DOF), F32)
        return jnp.concatenate([yref[:, cut], uref[:, cut], zero], axis=1)

    lane_of = lax.broadcasted_iota(jnp.int32, (1, LANES), 1)
    scale = jnp.where(lane_of < DOF, TWO_PI, to_u)
    shrink = jnp.where(lane_of < DOF, 1.0 / TWO_PI, 1.0 / to_u)
    first_lane = local * HS * (DOF + 1)
    own = rx[lax.axis_index("tm")][:, first_lane : first_lane + 2 * DOF]
    state = jnp.concatenate([own, jnp.zeros((epd, LANES - 2 * DOF), F32)], axis=1) * shrink
    xs[0] = state
    ends = sweep([packed(by, bu, n) for n in range(slices)], state)
    for n in range(slices):
        xs[n + 1] = ends[n]

    def iteration(k, corrections):
        for n in range(slices):
            cut = pl.ds(plan.where[n], DOF)
            ybuf[:, cut] = xs[n, :, 0:DOF]
            ubuf[:, cut] = xs[n, :, DOF : 2 * DOF]
        for j in range(HS):

            def substep(counter, carry):
                result = []
                for g, (base, width, first, count) in enumerate(plan.groups):
                    y, u = carry[g]
                    cut = pl.ds(base, width)
                    t = y - jnp.round(y)
                    s = t * t
                    poly = jnp.full_like(s, SIN[-1])
                    for c in SIN[-2::-1]:
                        poly = poly * s + c
                    force = (
                        tq[j, :, cut]
                        - spring[j, :, cut] * y
                        - fric[j, :, cut] * u
                        - (grav[:, cut] * t) * poly
                    )
                    u = u + product(force, g, width)
                    y = y + u
                    result.append((y, u))
                return tuple(result)

            first_state = tuple(
                (ybuf[:, pl.ds(base, width)], ubuf[:, pl.ds(base, width)])
                for base, width, first, count in plan.groups
            )
            last = lax.fori_loop(0, SUB, substep, first_state, unroll=unroll)
            for g, (base, width, first, count) in enumerate(plan.groups):
                ybuf[:, pl.ds(base, width)] = last[g][0]
                ubuf[:, pl.ds(base, width)] = last[g][1]
        worst = jnp.zeros((epd, 1), F32)
        changes = sweep([packed(ybuf, ubuf, n) - xs[n + 1] for n in range(slices)], None)
        for n in range(slices):
            real = changes[n] * scale
            worst = jnp.maximum(worst, jnp.sum(real * real, axis=1, keepdims=True))
            xs[n + 1] = xs[n + 1] + changes[n]
        return jnp.where(lane_of == k, jnp.sqrt(worst), corrections)

    corrections = lax.fori_loop(0, ITERS, iteration, jnp.zeros((epd, LANES), F32))
    rows_of = 2 * DOF
    for n in range(slices):
        dst, pos = divmod(n, local)
        out[dst, :, pos * rows_of : (pos + 1) * rows_of] = (xs[n + 1] * scale)[:, :rows_of]
    for dst in range(slices // local):
        out[dst, :, local * rows_of : local * rows_of + ITERS] = corrections[:, :ITERS]


def body(tm, env, init_state, torque, contact, mass_inverse, stiffness, damping, gravity,
         contact_stiffness, contact_damping):
    local = mass_inverse.shape[0]
    steps = torque.shape[0]
    env_local = init_state.shape[1]
    epd = env_local // tm
    slices = local * tm
    plan = Plan(slices)
    vmem = pl.BlockSpec(memory_space=pltpu.VMEM)
    dma = pltpu.SemaphoreType.DMA

    flat = jnp.concatenate(
        [torque.reshape(steps * DOF, env_local), contact.astype(F32), init_state], axis=0
    ).T
    wide = flat.shape[1]
    tx = flat.reshape(tm, epd, wide)
    m2 = mass_inverse.transpose(1, 0, 2).reshape(DOF, local * DOF)
    row = jnp.pad(jnp.sum(contact.astype(F32), axis=1)[None], ((0, 0), (0, LANES - steps)))
    rx, mall, rows = pl.pallas_call(
        functools.partial(exchange_in, tm, env),
        out_shape=(
            jax.ShapeDtypeStruct(tx.shape, F32),
            jax.ShapeDtypeStruct((tm,) + m2.shape, F32),
            jax.ShapeDtypeStruct((tm, env, 1, LANES), F32),
        ),
        in_specs=[vmem] * 3,
        out_specs=(vmem,) * 3,
        scratch_shapes=[dma((tm,))] * 4 + [dma((tm * env,))] * 2,
        compiler_params=pltpu.CompilerParams(collective_id=0, has_side_effects=True),
        name="exchange_in",
    )(tx, m2, row)

    prm = [p.reshape(1, DOF) for p in (stiffness, damping, gravity, contact_stiffness, contact_damping)]
    depth = -(-2 * DOF // 8) * 8
    lanes = plan.lanes
    groups = len(plan.groups)
    width_out = local * 2 * DOF + ITERS
    big = pltpu.VMEM((epd, lanes), F32)
    both = pltpu.VMEM((HS, epd, lanes), F32)
    thin = pltpu.VMEM((HS, 1, lanes), F32)
    out = pl.pallas_call(
        functools.partial(compute, slices, local, env_local * env),
        out_shape=jax.ShapeDtypeStruct((tm, epd, width_out), F32),
        in_specs=[vmem] * 8,
        out_specs=vmem,
        scratch_shapes=[
            both, both, both, pltpu.VMEM((1, lanes), F32), thin, thin,
            pltpu.VMEM((groups, WIDE, WIDE), BF16),
            pltpu.VMEM((LANES, LANES), F32),
            big, big, big, big,
            pltpu.VMEM((depth, lanes), F32), pltpu.VMEM((depth, lanes), F32),
            pltpu.VMEM((slices, 2 * LANES, 2 * LANES), BF16),
            pltpu.VMEM((slices, 2 * LANES, 2 * LANES), BF16),
            pltpu.VMEM((LANES, LANES), F32),
            pltpu.VMEM((slices + 1, epd, LANES), F32),
        ],
        name="parareal",
    )(rx, mall, rows, *prm)

    back = pl.pallas_call(
        functools.partial(exchange_out, tm),
        out_shape=jax.ShapeDtypeStruct(out.shape, F32),
        in_specs=[vmem],
        out_specs=vmem,
        scratch_shapes=[dma((tm,))] * 2,
        compiler_params=pltpu.CompilerParams(collective_id=1, has_side_effects=True),
        name="exchange_out",
    )(out)
    turned = back.reshape(env_local, width_out).T
    states = turned[: local * 2 * DOF].reshape(local, 2 * DOF, env_local)
    return states, turned[local * 2 * DOF :]


def solution(mesh):
    placed = (
        P(None, "env"),
        P("tm", None, "env"),
        P("tm", "env"),
        P("tm", None, None),
        P(),
        P(),
        P(),
        P(),
        P(),
    )
    return jax.shard_map(
        functools.partial(body, mesh.shape["tm"], mesh.shape["env"]),
        mesh=mesh,
        in_specs=placed,
        out_specs=(P("tm", None, "env"), P(None, "env")),
        check_vma=False,
    )
```
